256 devices in a mesh: samp: 8 (over z), seq: 32 (over x, y, core).
Axes of the slice: x: 4, y: 4, z: 8, core: 2. Of those that a mesh axis runs over, the one named last changes fastest.
Arguments:
- queries: bfloat16 [8, 16384, 3584], P('samp', 'seq'), may hold values from -200 to 200
- keys: bfloat16 [8, 16384, 512], P('samp', 'seq'), may hold values from -6 to 6
- values: bfloat16 [8, 16384, 512], P('samp', 'seq'), may hold values from -6 to 6
- reg_owner: int32 [8], P('samp'), may hold values from 0 to 31
- block_lists: int32 [8, 128, 8], P('samp', 'seq'), may hold values from 0 to 127, as said below
- list_counts: int32 [8, 128], P('samp', 'seq'), may hold values from 0 to 8, as said below
- image_blocks: int32 [8, 128], P('samp', 'seq'), may hold values from 0 to 1, as said below
Outputs:
- attended: bfloat16 [8, 16384, 3584], P('samp', 'seq')
The draws below stay inside these ranges and needn't reach their ends.
Inputs may be any that keep to these rules, and one draw needn't show every extreme that they name: `block_lists`: block b lies on sequence index b // 4. Entry t of a list is used only where t < the block's count, unused entries are 0. The used entries of one block name blocks of distinct sequence indices other than its own. Over all blocks of one sequence index, at most one distinct block of each other sequence index is named. On the last sequence index of each sample, the lists together name a block of every other index. `list_counts`: 0 for image blocks; at most 8. `image_blocks`: the blocks of the last sequence index of each sample are text blocks.
All inputs are finite; a program needn't handle non-finite values.
Results may differ from the reference program's by a relative error of at most 0.0043.
Values may be sent and summed in bfloat16 or wider, within the bound.
A program may use at most 128 MiB of HBM per device.

```python
import math
import jax
import jax.numpy as jnp
from jax import lax

QUERY_HEADS = 28
KEY_VALUE_HEADS = 4
HEAD_SIZE = 128
BLOCK_TOKENS = 128
REG = 64
LIST_ENTRIES = 8
BLK_DEV = 4
SAMPLE_COUNT = 8
TOK_DEV = 512
SAMPLE_BLOCKS = 128
SAMPLE_TOKENS = 16384
N_SEQ = 32


def activations(key):
    seeded = jax.random.fold_in(key, 11)
    key_queries, keys_for_keys = jax.random.split(seeded, 2)
    key_region = jnp.clip(jax.random.normal(keys_for_keys, (SAMPLE_COUNT, SAMPLE_TOKENS, KEY_VALUE_HEADS, HEAD_SIZE), jnp.float32), -6.0, 6.0)
    query_field = jnp.clip(jax.random.normal(key_queries, (SAMPLE_COUNT, SAMPLE_TOKENS, QUERY_HEADS, HEAD_SIZE), jnp.float32), -6.0, 6.0)
    query_out = query_field.reshape(SAMPLE_COUNT, SAMPLE_TOKENS, QUERY_HEADS * HEAD_SIZE).astype(jnp.bfloat16)
    key_output = key_region.reshape(SAMPLE_COUNT, SAMPLE_TOKENS, KEY_VALUE_HEADS * HEAD_SIZE).astype(jnp.bfloat16)
    return (query_out, key_output)


def draw_queries(key, part):
    return activations(key)[0]


def draw_keys(key, part):
    return activations(key)[1]


def layout(key):
    seeded = jax.random.fold_in(key, 7)
    key_kinds, key_chosen, key_order, key_counts = jax.random.split(seeded, 4)
    block_ids = jnp.arange(SAMPLE_BLOCKS, dtype=jnp.int32)
    block_device = block_ids // BLK_DEV
    local_ids = block_ids % BLK_DEV
    last_device = N_SEQ - 1
    kinds = (jax.random.randint(key_kinds, (SAMPLE_COUNT, SAMPLE_BLOCKS), 0, 4, jnp.int32) == 0).astype(jnp.int32)
    kinds = jnp.where(block_device[None, :] == last_device, 0, kinds)
    chosen = jax.random.randint(key_chosen, (SAMPLE_COUNT, N_SEQ, N_SEQ), 0, BLK_DEV, jnp.int32)
    owner_ids = jnp.arange(N_SEQ, dtype=jnp.int32)
    ranking = jax.random.randint(key_order, (SAMPLE_COUNT, SAMPLE_BLOCKS, N_SEQ), 0, 2 ** 16, jnp.int32) * N_SEQ + owner_ids
    ranking = jnp.where(owner_ids[None, None, :] != block_device[None, :, None], ranking, 2 ** 30)
    ordered = jnp.argsort(ranking, axis=-1)[..., :LIST_ENTRIES].astype(jnp.int32)
    slot_ids = jnp.arange(LIST_ENTRIES, dtype=jnp.int32)
    full_count = min(LIST_ENTRIES, N_SEQ - 1)
    cyclic = (local_ids[:, None] * full_count + slot_ids[None, :]) % (N_SEQ - 1)
    is_last = block_device == last_device
    ordered = jnp.where(is_last[None, :, None], cyclic[None], ordered)
    counts = full_count - jax.random.randint(key_counts, (SAMPLE_COUNT, SAMPLE_BLOCKS), 0, 3, jnp.int32)
    counts = jnp.where(is_last[None, :], full_count, counts)
    counts = jnp.where(kinds == 1, 0, counts)
    chosen_rows = chosen[:, block_device, :]
    picked = jnp.take_along_axis(chosen_rows, ordered, axis=2)
    list_ids = ordered * BLK_DEV + picked
    list_ids = jnp.where(slot_ids[None, None, :] < counts[..., None], list_ids, 0)
    return (list_ids.astype(jnp.int32), counts.astype(jnp.int32), kinds.astype(jnp.int32))


def draw_block_lists(key, part):
    return layout(key)[0]


def draw_list_counts(key, part):
    return layout(key)[1]


def draw_image_blocks(key, part):
    return layout(key)[2]


def place_ends(result, key, smallest, high):
    index_at = [jax.random.randint(jax.random.fold_in(key, axis), (), 0, length) for axis, length in enumerate(result.shape)]
    widest = result.shape.index(max(result.shape))
    beside = index_at[:widest] + [(index_at[widest] + 1) % result.shape[widest]] + index_at[widest + 1:]
    return result.at[tuple(index_at)].set(smallest).at[tuple(beside)].set(high)


def shard_levels(own_key, shape, cuts, low, high):
    gain = 1.0
    for dim, blocks in cuts:
        heights = jax.random.uniform(jax.random.fold_in(jax.random.fold_in(own_key, 6), dim), (blocks,), jnp.float32, low / len(cuts), high / len(cuts))
        gain = gain * jnp.repeat(jnp.exp(heights), shape[dim] // blocks).reshape((-1,) + (1,) * (len(shape) - 1 - dim))
    return gain


def normal_values(key, extent, width, most, pieces=(), kind=jnp.bfloat16):
    drawn = width * jax.random.normal(key, extent, jnp.float32)
    if pieces:
        drawn = drawn * shard_levels(key, extent, pieces, -0.22, 0.18)
    return jnp.clip(drawn, -most, most).astype(kind)


def setup_inputs(seed: int = 0) -> dict:
    splits = jax.random.split(jax.random.key(seed), 8)
    return {
        "queries": draw_queries(jax.random.fold_in(splits[7], 71), 0),
        "keys": draw_keys(jax.random.fold_in(splits[7], 71), 0),
        "values": normal_values(splits[2], (SAMPLE_COUNT, SAMPLE_TOKENS, KEY_VALUE_HEADS * HEAD_SIZE), 1.0, 6.0, ((0, 8), (1, 32))),
        "reg_owner": place_ends(jax.random.randint(splits[3], (SAMPLE_COUNT,), 0, N_SEQ), jax.random.fold_in(splits[3], 1), 0, N_SEQ - 1).astype(jnp.int32),
        "block_lists": draw_block_lists(jax.random.fold_in(splits[7], 71), 0),
        "list_counts": draw_list_counts(jax.random.fold_in(splits[7], 71), 0),
        "image_blocks": draw_image_blocks(jax.random.fold_in(splits[7], 71), 0),
    }


very_low = -1e+30

def group_part(query_row_list, key_row_list, value_row_list, visible):
    head_grouped = query_row_list.astype(jnp.float32).reshape(BLOCK_TOKENS, KEY_VALUE_HEADS, QUERY_HEADS // KEY_VALUE_HEADS, HEAD_SIZE)
    per_head_keys = key_row_list.astype(jnp.float32).reshape(-1, KEY_VALUE_HEADS, HEAD_SIZE)
    per_head_values = value_row_list.astype(jnp.float32).reshape(-1, KEY_VALUE_HEADS, HEAD_SIZE)
    scores = jnp.einsum('qhgd,khd->hgqk', head_grouped, per_head_keys) / math.sqrt(HEAD_SIZE)
    scores = jnp.where(visible, scores, very_low)
    maxima = lax.optimization_barrier(jnp.max(scores, axis=-1))
    weights = jnp.where(visible, jnp.exp(scores - maxima[..., None]), 0.0)
    totals = lax.optimization_barrier(jnp.sum(weights, axis=-1))
    rounded = lax.optimization_barrier(weights.astype(jnp.bfloat16)).astype(jnp.float32)
    partial_value = jnp.einsum('hgqk,khd->hgqd', rounded, per_head_values)
    return (maxima, totals, partial_value)

def combine(parts):
    top_score = jnp.maximum(jnp.maximum(parts[0][0], parts[1][0]), parts[2][0])
    numerator = jnp.zeros(parts[0][2].shape, jnp.float32)
    denominator = jnp.zeros(parts[0][1].shape, jnp.float32)
    for maxima, totals, partial_value in parts:
        rescale = jnp.exp(maxima - top_score)
        numerator = numerator + rescale[..., None] * partial_value
        denominator = denominator + rescale * totals
    merged = numerator / denominator[..., None]
    return merged.transpose(2, 0, 1, 3).reshape(merged.shape[2], -1)

def reference(queries, keys, values, reg_owner, block_lists, list_counts, image_blocks):
    outputs = []
    row_ids = jnp.arange(BLOCK_TOKENS)
    slot_rows = jnp.arange(LIST_ENTRIES * BLOCK_TOKENS) // BLOCK_TOKENS
    for sample in range(SAMPLE_COUNT):
        query_all = queries[sample]
        every_key = keys[sample]
        every_value = values[sample]
        blocked_keys = every_key.reshape(SAMPLE_BLOCKS, BLOCK_TOKENS, KEY_VALUE_HEADS * HEAD_SIZE)
        blocked_values = every_value.reshape(SAMPLE_BLOCKS, BLOCK_TOKENS, KEY_VALUE_HEADS * HEAD_SIZE)
        reg_start = (reg_owner[sample] * TOK_DEV).astype(jnp.int32)
        reg_keys = lax.dynamic_slice_in_dim(every_key, reg_start, REG, 0)
        reg_values = lax.dynamic_slice_in_dim(every_value, reg_start, REG, 0)
        sample_lists = block_lists[sample]
        sample_counts = list_counts[sample]
        sample_image = image_blocks[sample]

        def one_block(block_id):
            row_start = (block_id * BLOCK_TOKENS).astype(jnp.int32)
            query_row_list = lax.dynamic_slice_in_dim(query_all, row_start, BLOCK_TOKENS, 0)
            own_keys = lax.dynamic_slice_in_dim(every_key, row_start, BLOCK_TOKENS, 0)
            own_values = lax.dynamic_slice_in_dim(every_value, row_start, BLOCK_TOKENS, 0)
            listed_block_index = sample_lists[block_id]
            remote_keys = blocked_keys[listed_block_index].reshape(LIST_ENTRIES * BLOCK_TOKENS, KEY_VALUE_HEADS * HEAD_SIZE)
            remote_values = blocked_values[listed_block_index].reshape(LIST_ENTRIES * BLOCK_TOKENS, KEY_VALUE_HEADS * HEAD_SIZE)
            reg_visible = jnp.ones((BLOCK_TOKENS, REG), bool)
            own_visible = (row_ids[None, :] <= row_ids[:, None]) | (sample_image[block_id] == 1)
            far_visible = jnp.broadcast_to(slot_rows[None, :] < sample_counts[block_id], (BLOCK_TOKENS, LIST_ENTRIES * BLOCK_TOKENS))
            parts = [group_part(query_row_list, reg_keys, reg_values, reg_visible), group_part(query_row_list, own_keys, own_values, own_visible), group_part(query_row_list, remote_keys, remote_values, far_visible)]
            return combine(parts).astype(jnp.bfloat16)
        blocks_out = lax.map(one_block, jnp.arange(SAMPLE_BLOCKS, dtype=jnp.int32))
        outputs.append(blocks_out.reshape(SAMPLE_TOKENS, QUERY_HEADS * HEAD_SIZE))
    return jnp.stack(outputs)
```

```python
import math

import jax
import jax.numpy as jnp
from jax import lax
from jax.experimental import pallas as pl
from jax.experimental.pallas import tpu as pltpu
from jax.sharding import PartitionSpec as P

QUERY_HEADS = 28
KEY_VALUE_HEADS = 4
HEAD_SIZE = 128
REG = 64
GROUP = QUERY_HEADS // KEY_VALUE_HEADS
SCALE = math.log2(math.e) / math.sqrt(HEAD_SIZE)


very_low = -1e30


def from_root(array, axis, root):
    return lax.dynamic_index_in_dim(lax.all_gather(array, axis), root, 0, keepdims=False)


def gather_together(arrays, axis):
    flat = jnp.concatenate([a.reshape(-1) for a in arrays])
    lines, at, done = (lax.all_gather(flat, axis), 0, [])
    for a in arrays:
        tiles = lines[:, at : at + a.size].reshape(-1, *a.shape[1:])
        done.append(tiles)
        at += a.size
    return tuple(done)


def dot_t(a, b):
    return lax.dot_general(a, b, (((1,), (1,)), ((), ())), preferred_element_type=jnp.float32)


def attend(q, reg_k, reg_v, own_k, own_v, far, is_image):
    rows = q.shape[0]
    stacked = jnp.concatenate(
        [q[:, g * HEAD_SIZE : (g + 1) * HEAD_SIZE] for g in range(GROUP)], axis=0
    )
    reg_keys = jnp.concatenate([reg_k, reg_k], axis=0)
    zero = jnp.zeros((rows, HEAD_SIZE), jnp.bfloat16)
    ones = jnp.ones((rows, HEAD_SIZE), jnp.bfloat16)
    half = jnp.concatenate([ones[:REG], zero[:REG]], axis=0)
    reg_values = jnp.concatenate([reg_v, zero[:REG]], axis=0)
    slots = [(own_k, own_v, ones), (reg_keys, reg_values, half)]
    for k, v, used in far:
        slots.append(
            (jnp.where(used, k, reg_keys), jnp.where(used, v, zero), jnp.where(used, ones, zero))
        )
    visible = (
        lax.broadcasted_iota(jnp.int32, (rows, rows), 1)
        <= lax.broadcasted_iota(jnp.int32, (rows, rows), 0)
    ) | is_image
    seen = jnp.concatenate([visible] * GROUP, axis=0)
    scores = []
    for i in range(0, len(slots), 2):
        scores.append(dot_t(stacked, jnp.concatenate([slots[i][0], slots[i + 1][0]], axis=0)))
    scores[0] = jnp.concatenate(
        [jnp.where(seen, scores[0][:, :rows], very_low), scores[0][:, rows:]], axis=1
    )
    top = scores[0]
    for s in scores[1:]:
        top = jnp.maximum(top, s)
    top = jnp.max(top, axis=1, keepdims=True)
    total = None
    for i, s in enumerate(scores):
        weights = jnp.exp2((s - top) * SCALE).astype(jnp.bfloat16)
        a, b = slots[2 * i], slots[2 * i + 1]
        rhs = jnp.concatenate(
            [jnp.concatenate([a[1], a[2]], axis=1), jnp.concatenate([b[1], b[2]], axis=1)], axis=0
        )
        part = jnp.dot(weights, rhs, preferred_element_type=jnp.float32)
        total = part if total is None else total + part
    merged = (total[:, :HEAD_SIZE] / total[:, HEAD_SIZE:]).astype(jnp.bfloat16)
    return jnp.concatenate([merged[g * rows : (g + 1) * rows] for g in range(GROUP)], axis=1)


def attention_kernel(
    place, counts, image, q_ref, k_ref, v_ref, reg_ref, far_k_ref, far_v_ref, out_ref
):
    b = pl.program_id(1)
    far = []
    for t in range(8):
        j = place[b, t]
        far.append((far_k_ref[j], far_v_ref[j], t < counts[b]))
    out_ref[...] = attend(
        q_ref[...], reg_ref[0], reg_ref[1], k_ref[...], v_ref[...], far, image[b] == 1
    )


def attention(q, k, v, registers, far_k, far_v, place, counts, image):
    blocks = place.shape[0]
    rows = q.shape[0] // blocks
    width = GROUP * HEAD_SIZE
    devices = far_k.shape[0]
    return pl.pallas_call(
        attention_kernel,
        out_shape=jax.ShapeDtypeStruct(q.shape, jnp.bfloat16),
        grid_spec=pltpu.PrefetchScalarGridSpec(
            num_scalar_prefetch=3,
            grid=(KEY_VALUE_HEADS, blocks),
            in_specs=[
                pl.BlockSpec((rows, width), lambda h, b, *_: (b, h)),
                pl.BlockSpec((rows, HEAD_SIZE), lambda h, b, *_: (b, h)),
                pl.BlockSpec((rows, HEAD_SIZE), lambda h, b, *_: (b, h)),
                pl.BlockSpec((2, REG, HEAD_SIZE), lambda h, b, *_: (0, 0, h)),
                pl.BlockSpec((devices, rows, HEAD_SIZE), lambda h, b, *_: (0, 0, h)),
                pl.BlockSpec((devices, rows, HEAD_SIZE), lambda h, b, *_: (0, 0, h)),
            ],
            out_specs=pl.BlockSpec((rows, width), lambda h, b, *_: (b, h)),
        ),
        compiler_params=pltpu.CompilerParams(vmem_limit_bytes=56 << 20),
        name="attention",
    )(place, counts, image, q, k, v, registers, far_k, far_v)


def per_device(queries, keys, values, reg_owner, block_lists, list_counts, image_blocks):
    every_key = keys[0]
    every_value = values[0]
    local_lists = block_lists[0]
    local_counts = list_counts[0]
    devices = lax.axis_size("seq")
    position = lax.axis_index("seq")
    blocks_here = local_lists.shape[0]
    slot_count = local_lists.shape[1]
    rows_block = every_key.shape[0] // blocks_here
    kv_width = every_key.shape[1]
    stacked = jnp.stack([every_key[:REG], every_value[:REG]])
    registers = from_root(stacked, "seq", reg_owner[0])
    all_lists, all_counts = gather_together((local_lists, local_counts), "seq")
    own_ids = position * blocks_here + jnp.arange(blocks_here, dtype=jnp.int32)
    live_slots = jnp.arange(slot_count, dtype=jnp.int32)[None, :] < all_counts[:, None]
    named_here = (all_lists[:, :, None] == own_ids[None, None, :]) & live_slots[:, :, None]
    wanted = jnp.any(named_here, axis=1).reshape(devices, blocks_here, blocks_here)
    selector = jnp.any(wanted, axis=1).astype(jnp.bfloat16)
    exchanged = []
    for array in (every_key, every_value):
        sent = jnp.dot(
            selector,
            array.reshape(blocks_here, rows_block * kv_width),
            preferred_element_type=jnp.float32,
        ).astype(jnp.bfloat16)
        exchanged.append(
            lax.all_to_all(
                sent.reshape(devices, rows_block, kv_width),
                "seq",
                split_axis=0,
                concat_axis=0,
                tiled=True,
            )
        )
    out = attention(
        queries[0],
        every_key,
        every_value,
        registers,
        exchanged[0],
        exchanged[1],
        local_lists // blocks_here,
        local_counts,
        image_blocks[0],
    )
    return out[None]


def solution(mesh):
    placed = (
        P("samp", "seq", None),
        P("samp", "seq", None),
        P("samp", "seq", None),
        P("samp"),
        P("samp", "seq", None),
        P("samp", "seq"),
        P("samp", "seq"),
    )
    return jax.shard_map(
        per_device, mesh=mesh, in_specs=placed, out_specs=P("samp", "seq", None), check_vma=False
    )
```

```python
import math

import jax
import jax.numpy as jnp
from jax import lax
from jax.experimental import pallas as pl
from jax.experimental.pallas import tpu as pltpu
from jax.sharding import PartitionSpec as P

QUERY_HEADS = 28
KEY_VALUE_HEADS = 4
HEAD_SIZE = 128
REG = 64
GROUP = QUERY_HEADS // KEY_VALUE_HEADS
SCALE = math.log2(math.e) / math.sqrt(HEAD_SIZE)


very_low = -1e30


def dot_t(a, b):
    return lax.dot_general(a, b, (((1,), (1,)), ((), ())), preferred_element_type=jnp.float32)


def attend(q, reg_k, reg_v, own_k, own_v, far, is_image):
    rows = q.shape[0]
    stacked = jnp.concatenate(
        [q[:, g * HEAD_SIZE : (g + 1) * HEAD_SIZE] for g in range(GROUP)], axis=0
    )
    reg_keys = jnp.concatenate([reg_k, reg_k], axis=0)
    zero = jnp.zeros((rows, HEAD_SIZE), jnp.bfloat16)
    ones = jnp.ones((rows, HEAD_SIZE), jnp.bfloat16)
    half = jnp.concatenate([ones[:REG], zero[:REG]], axis=0)
    reg_values = jnp.concatenate([reg_v, zero[:REG]], axis=0)
    slots = [(own_k, own_v, ones), (reg_keys, reg_values, half)]
    slots += far
    visible = lax.broadcasted_iota(jnp.int32, (rows, rows), 1) <= (
        lax.broadcasted_iota(jnp.int32, (rows, rows), 0) + is_image * rows
    )
    seen = jnp.concatenate([visible] * GROUP, axis=0)
    scores = []
    for i in range(0, len(slots), 2):
        scores.append(dot_t(stacked, jnp.concatenate([slots[i][0], slots[i + 1][0]], axis=0)))
    scores[0] = jnp.concatenate(
        [jnp.where(seen, scores[0][:, :rows], very_low), scores[0][:, rows:]], axis=1
    )
    top = scores[0]
    for s in scores[1:]:
        top = jnp.maximum(top, s)
    top = jnp.max(top, axis=1, keepdims=True)
    total = None
    for i, s in enumerate(scores):
        weights = jnp.exp2((s - top) * SCALE).astype(jnp.bfloat16)
        a, b = slots[2 * i], slots[2 * i + 1]
        rhs = jnp.concatenate(
            [jnp.concatenate([a[1], a[2]], axis=1), jnp.concatenate([b[1], b[2]], axis=1)], axis=0
        )
        part = jnp.dot(weights, rhs, preferred_element_type=jnp.float32)
        total = part if total is None else total + part
    merged = (total[:, :HEAD_SIZE] / total[:, HEAD_SIZE:]).astype(jnp.bfloat16)
    return jnp.concatenate([merged[g * rows : (g + 1) * rows] for g in range(GROUP)], axis=1)


SIDE = 4
CORES = 2
SENDERS = SIDE * CORES


def layer_kernel(
    q_hbm,
    k_hbm,
    v_hbm,
    lists,
    counts,
    image,
    owner,
    out_hbm,
    q_here,
    out_here,
    gk0,
    gk1,
    gk2,
    gk3,
    gv0,
    gv1,
    gv2,
    gv3,
    rk0,
    rk1,
    rk2,
    rk3,
    rv0,
    rv1,
    rv2,
    rv3,
    outgoing,
    passing,
    asks_a,
    asks_b,
    asks_a_s,
    asks_b_s,
    marks,
    table_sem,
    load_sem,
    q_sem,
    out_sem,
    ask_send,
    ask_recv,
    ring_send,
    ring_recv,
    sel_send,
    sel_recv,
    pass_send,
    pass_recv,
):
    gathered = ((gk0, gk1, gk2, gk3), (gv0, gv1, gv2, gv3))
    received = ((rk0, rk1, rk2, rk3), (rv0, rv1, rv2, rv3))
    samp = lax.axis_index("samp")
    me = lax.axis_index("seq")
    x = me // SENDERS
    y = (me // CORES) % SIDE
    k = me % CORES
    blocks, slots = lists.shape
    rows = k_hbm.shape[0] * k_hbm.shape[1] // blocks
    width = GROUP * HEAD_SIZE

    def flag(b, t):
        return jnp.minimum(jnp.maximum(counts[b] - t, 0), 1)

    def device(c, place, core):
        if c == 0:
            return x * SENDERS + place * CORES + core
        return place * SENDERS + y * CORES + core

    def source(c, place):
        if c == 0:
            return place * SENDERS + y * CORES + k
        return x * SENDERS + place * CORES + k

    first = (x, y)
    second = (y, x)
    mine = (y * CORES + k, x * CORES + k)

    def remote(src, dst, send_sem, recv_sem, target):
        return pltpu.make_async_remote_copy(
            src_ref=src,
            dst_ref=dst,
            send_sem=send_sem,
            recv_sem=recv_sem,
            device_id=(samp, target),
            device_id_type=pl.DeviceIdType.MESH,
        )

    def load(c, h):
        hbm = (k_hbm, v_hbm)[c]
        return pltpu.make_async_copy(
            hbm.at[:, :, pl.ds(h * HEAD_SIZE, HEAD_SIZE)],
            gathered[c][h].at[first[c]],
            load_sem.at[c, h],
        )

    def load_q(h):
        cols = pl.ds(h * width, width)
        return pltpu.make_async_copy(q_hbm.at[:, cols], q_here.at[:, cols], q_sem.at[h])

    for h in range(KEY_VALUE_HEADS):
        for c in range(2):
            load(c, h).start()
    for h in range(KEY_VALUE_HEADS):
        load_q(h).start()

    lanes = lax.broadcasted_iota(jnp.int32, (1, 128), 1)
    asks = jnp.zeros((1, 128), jnp.int32)
    for b in range(blocks):
        for t in range(slots):
            entry = lists[b, t]
            used = flag(b, t)
            asks = jnp.where(lanes == (entry >> 2) * used + used - 1, entry & 3, asks)
    marks[0] = jnp.zeros((rows, HEAD_SIZE), jnp.bfloat16)
    marks[1] = jnp.ones((rows, HEAD_SIZE), jnp.bfloat16)
    asks_a[mine[0]] = asks
    asks_b[mine[1]] = asks

    barrier = pltpu.get_barrier_semaphore()
    greeted = []
    for i in range(1, SENDERS):
        greeted.append(x * SENDERS + (mine[0] + i) % SENDERS)
    for i in range(1, SIDE):
        for core in range(CORES):
            greeted.append(((x + i) % SIDE) * SENDERS + y * CORES + core)
    for target in greeted:
        pl.semaphore_signal(
            barrier, inc=1, device_id=(samp, target), device_id_type=pl.DeviceIdType.MESH
        )
    pl.semaphore_wait(barrier, len(greeted))

    tables = (asks_a, asks_b)

    def ask(c, other):
        return remote(
            tables[c].at[mine[c]],
            tables[c].at[mine[c]],
            ask_send.at[c, other],
            ask_recv.at[c, mine[c]],
            device(c, other // CORES, other % CORES),
        )

    for c in range(2):
        for i in range(1, SENDERS):
            ask(c, (mine[c] + i) % SENDERS).start()

    def ring(c, h, kind):
        step = 1 if kind % 2 == 0 else -1
        at = first[c]
        ref = gathered[c][h]
        if kind < 2:
            part = ref.at[at]
        else:
            part = ref.at[(at - step) % SIDE, pl.ds((kind - 2) * blocks, blocks)]
        return remote(
            part,
            part,
            ring_send.at[c, h, kind],
            ring_recv.at[c, h, kind],
            source(c, (at + step) % SIDE),
        )

    def ring_arrived(c, h, kind):
        step = 1 if kind % 2 == 0 else -1
        at = first[c]
        ref = gathered[c][h]
        if kind < 2:
            part = ref.at[(at - step) % SIDE]
        else:
            part = ref.at[(at - 2 * step) % SIDE, pl.ds((kind - 2) * blocks, blocks)]
        remote(
            part,
            part,
            ring_send.at[c, h, kind],
            ring_recv.at[c, h, kind],
            source(c, (at + step) % SIDE),
        ).wait_recv()

    def start_ring(h):
        for c in range(2):
            load(c, h).wait()
            ring(c, h, 0).start()
            ring(c, h, 1).start()

    def pass_ring(h):
        for kind in range(2):
            for c in range(2):
                ring_arrived(c, h, kind)
                ring(c, h, kind + 2).start()

    root = owner[0]
    reg_place = (root >> 3, (root >> 1) & 3)
    reg_sender = (root & 7, (root >> 3) * CORES + (root & 1))

    def first_leg(c, h, way):
        step = 1 if way == 0 else -1
        at = second[c]
        return remote(
            outgoing.at[c, h, ((at + 2) % SIDE) * CORES + way],
            passing.at[c, h, way],
            pass_send.at[c, h, way],
            pass_recv.at[c, h, way],
            device(c, (at + step) % SIDE, k),
        )

    def direct(c, h, role):
        at = second[c]
        if role == 4:
            place, core = at, 1 - k
        else:
            place, core = (at + (1 if role < 2 else -1)) % SIDE, role % CORES
        return remote(
            outgoing.at[c, h, place * CORES + core],
            received[c][h].at[mine[c]],
            sel_send.at[c, h, role],
            sel_recv.at[c, h, mine[c]],
            device(c, place, core),
        )

    def last_leg(c, h, way):
        step = 1 if way == 0 else -1
        at = second[c]
        origin = ((at - step) % SIDE) * CORES + k
        return remote(
            passing.at[c, h, way],
            received[c][h].at[origin],
            sel_send.at[c, h, 5 + way],
            sel_recv.at[c, h, origin],
            device(c, (at + step) % SIDE, way),
        )

    def select(h):
        for c in range(2):
            ring_arrived(c, h, 2)
            ring_arrived(c, h, 3)
        for c in range(2):
            ref = gathered[c][h]
            table = (asks_a_s, asks_b_s)[c]
            spots = [source(c, s) for s in range(SIDE)]

            @pl.loop(0, SENDERS)
            def _(d):
                for s in range(SIDE):
                    wanted = table[d, 0, spots[s]]
                    outgoing[c, h, d, 2 * s] = ref[s, 2 * wanted]
                    outgoing[c, h, d, 2 * s + 1] = ref[s, 2 * wanted + 1]
                outgoing[c, h, d, 2 * SIDE] = ref[reg_place[c], 0]

        for c in range(2):
            first_leg(c, h, 0).start()
            first_leg(c, h, 1).start()
        for role in range(5):
            for c in range(2):
                direct(c, h, role).start()
        for c in range(2):
            received[c][h][mine[c]] = outgoing[c, h, mine[c]]

    def pass_on(h):
        for way in range(2):
            for c in range(2):
                first_leg(c, h, way).wait_recv()
                last_leg(c, h, way).start()

    def all_here(h):
        load_q(h).wait()
        for c in range(2):
            for i in range(1, SENDERS):
                origin = (mine[c] + i) % SENDERS
                remote(
                    received[c][h].at[origin],
                    received[c][h].at[origin],
                    sel_send.at[c, h, 0],
                    sel_recv.at[c, h, origin],
                    device(c, origin // CORES, origin % CORES),
                ).wait_recv()
        for i in range(2):
            received[0][h][SENDERS, i] = received[0][h][reg_sender[0], 2 * SIDE]
            received[1][h][SENDERS, i] = jnp.zeros((REG, HEAD_SIZE), jnp.bfloat16)

    def store(h, b):
        return pltpu.make_async_copy(
            out_here.at[h * blocks + b],
            out_hbm.at[pl.ds(pl.multiple_of(b * rows, rows), rows), pl.ds(h * width, width)],
            out_sem.at[h * blocks + b],
        )

    def whole(ref, i, j):
        return jnp.concatenate([ref[i, 2 * j], ref[i, 2 * j + 1]], axis=0)

    def compute(h, start, stop):
        keys, values = received[0][h], received[1][h]

        @pl.loop(start, stop)
        def _(b):
            here = pl.ds(pl.multiple_of(b * rows, rows), rows)
            far = []
            for t in range(slots):
                o = lists[b, t] >> 2
                used = flag(b, t)
                spare = SENDERS * (1 - used)
                ox, oy, ok = o >> 3, (o >> 1) & 3, o & 1
                far.append(
                    (
                        whole(keys, (o & 7) * used + spare, ox * used),
                        whole(values, (ox * CORES + ok) * used + spare, oy * used),
                        marks[used],
                    )
                )
            out_here[h * blocks + b] = attend(
                q_here[here, pl.ds(h * width, width)],
                keys[reg_sender[0], 2 * SIDE],
                values[reg_sender[1], 2 * SIDE],
                whole(gathered[0][h], x, b),
                whole(gathered[1][h], y, b),
                far,
                image[b],
            )
            store(h, b).start()

    half = blocks // 2
    start_ring(0)
    start_ring(1)
    pass_ring(0)
    start_ring(2)
    pass_ring(1)
    start_ring(3)
    for c in range(2):
        for i in range(1, SENDERS):
            other = (mine[c] + i) % SENDERS
            remote(
                tables[c].at[other],
                tables[c].at[other],
                ask_send.at[c, other],
                ask_recv.at[c, other],
                device(c, other // CORES, other % CORES),
            ).wait_recv()
    to_scalars = (
        pltpu.make_async_copy(asks_a, asks_a_s, table_sem.at[0]),
        pltpu.make_async_copy(asks_b, asks_b_s, table_sem.at[1]),
    )
    for copy in to_scalars:
        copy.start()
    for copy in to_scalars:
        copy.wait()
    select(0)
    pass_ring(2)
    pass_on(0)
    pass_ring(3)
    select(1)
    for h in range(KEY_VALUE_HEADS):
        all_here(h)
        compute(h, 0, half)
        if h + 1 < KEY_VALUE_HEADS:
            pass_on(h + 1)
        if h + 2 < KEY_VALUE_HEADS:
            select(h + 2)
        compute(h, half, blocks)

    for c in range(2):
        for i in range(1, SENDERS):
            ask(c, (mine[c] + i) % SENDERS).wait_send()
    for h in range(KEY_VALUE_HEADS):
        for c in range(2):
            for kind in range(4):
                ring(c, h, kind).wait_send()
            for way in range(2):
                first_leg(c, h, way).wait_send()
                last_leg(c, h, way).wait_send()
            for role in range(5):
                direct(c, h, role).wait_send()
        for b in range(blocks):
            store(h, b).wait()


def layer(q, k, v, lists, counts, image, owner):
    blocks = lists.shape[0]
    rows = q.shape[0] // blocks
    width = GROUP * HEAD_SIZE
    message = (2 * SIDE + 1, REG, HEAD_SIZE)
    k = k.reshape(-1, REG, k.shape[1])
    v = v.reshape(-1, REG, v.shape[1])
    heads = KEY_VALUE_HEADS
    bf16 = jnp.bfloat16
    dma = pltpu.SemaphoreType.DMA
    return pl.pallas_call(
        layer_kernel,
        out_shape=jax.ShapeDtypeStruct(q.shape, bf16),
        in_specs=[pl.BlockSpec(memory_space=pl.ANY)] * 3
        + [pl.BlockSpec(memory_space=pltpu.SMEM)] * 4,
        out_specs=pl.BlockSpec(memory_space=pl.ANY),
        scratch_shapes=[
            pltpu.VMEM(q.shape, bf16),
            pltpu.VMEM((heads * blocks, rows, width), bf16),
        ]
        + [pltpu.VMEM((SIDE, 2 * blocks, REG, HEAD_SIZE), bf16)] * 8
        + [pltpu.VMEM((SENDERS + 1, *message), bf16)] * 8
        + [
            pltpu.VMEM((2, heads, SENDERS, *message), bf16),
            pltpu.VMEM((2, heads, 2, *message), bf16),
            pltpu.VMEM((SENDERS, 1, 128), jnp.int32),
            pltpu.VMEM((SENDERS, 1, 128), jnp.int32),
            pltpu.SMEM((SENDERS, 1, 128), jnp.int32),
            pltpu.SMEM((SENDERS, 1, 128), jnp.int32),
            pltpu.VMEM((2, rows, HEAD_SIZE), bf16),
            dma((2,)),
            dma((2, heads)),
            dma((heads,)),
            dma((heads * blocks,)),
            dma((2, SENDERS)),
            dma((2, SENDERS)),
            dma((2, heads, 4)),
            dma((2, heads, 4)),
            dma((2, heads, 7)),
            dma((2, heads, SENDERS)),
            dma((2, heads, 2)),
            dma((2, heads, 2)),
        ],
        compiler_params=pltpu.CompilerParams(
            collective_id=0, has_side_effects=True, vmem_limit_bytes=60 << 20
        ),
        name="layer",
    )(q, k, v, lists, counts, image, owner)


def per_device(queries, keys, values, reg_owner, block_lists, list_counts, image_blocks):
    out = layer(
        queries[0],
        keys[0],
        values[0],
        block_lists[0],
        list_counts[0],
        image_blocks[0],
        reg_owner,
    )
    return out[None]


def solution(mesh):
    placed = (
        P("samp", "seq", None),
        P("samp", "seq", None),
        P("samp", "seq", None),
        P("samp"),
        P("samp", "seq", None),
        P("samp", "seq"),
        P("samp", "seq"),
    )
    return jax.shard_map(
        per_device, mesh=mesh, in_specs=placed, out_specs=P("samp", "seq", None), check_vma=False
    )
```

```python
import math

import jax
import jax.numpy as jnp
from jax import lax
from jax.experimental import pallas as pl
from jax.experimental.pallas import tpu as pltpu
from jax.sharding import PartitionSpec as P

QUERY_HEADS = 28
KEY_VALUE_HEADS = 4
HEAD_SIZE = 128
REG = 64
GROUP = QUERY_HEADS // KEY_VALUE_HEADS
SCALE = math.log2(math.e) / math.sqrt(HEAD_SIZE)


very_low = -1e30


def dot_t(a, b):
    return lax.dot_general(a, b, (((1,), (1,)), ((), ())), preferred_element_type=jnp.float32)


PARTS = 4


def stacked_heads(q):
    return jnp.concatenate(
        [q[:, g * HEAD_SIZE : (g + 1) * HEAD_SIZE] for g in range(GROUP)], axis=0
    )


def spread_heads(merged, rows):
    return jnp.concatenate([merged[g * rows : (g + 1) * rows] for g in range(GROUP)], axis=1)


def paired(blocks):
    return [
        jnp.concatenate([blocks[i], blocks[i + 1]], axis=0) for i in range(0, len(blocks), 2)
    ]


def key_pairs(own_k, reg_k, far):
    return paired([own_k, jnp.concatenate([reg_k, reg_k], axis=0)] + far)


def value_pairs(own_v, reg_v, far, used):
    rows = own_v.shape[0]
    zero = jnp.zeros((rows, HEAD_SIZE), jnp.bfloat16)
    ones = jnp.ones((rows, HEAD_SIZE), jnp.bfloat16)
    half = jnp.concatenate([ones[:REG], zero[:REG]], axis=0)
    values = [own_v, jnp.concatenate([reg_v, zero[:REG]], axis=0)] + far
    marks = [ones, half] + used
    return paired([jnp.concatenate([v, m], axis=1) for v, m in zip(values, marks)])


def seen_rows(rows, is_image):
    visible = lax.broadcasted_iota(jnp.int32, (rows, rows), 1) <= (
        lax.broadcasted_iota(jnp.int32, (rows, rows), 0) + is_image * rows
    )
    return jnp.concatenate([visible] * GROUP, axis=0)


def score(stacked, keys, seen, lo, hi):
    rows = seen.shape[1]
    scores = [dot_t(stacked[lo:hi], key) for key in keys]
    own = jnp.where(seen[lo:hi], scores[0][:, :rows], very_low)
    scores[0] = jnp.concatenate([own, scores[0][:, rows:]], axis=1)
    return scores


def soften(scores):
    top = scores[0]
    for s in scores[1:]:
        top = jnp.maximum(top, s)
    top = jnp.max(top, axis=1, keepdims=True)
    return [jnp.exp2((s - top) * SCALE).astype(jnp.bfloat16) for s in scores]


def finish(weights, values):
    total = None
    for w, value in zip(weights, values):
        part = jnp.dot(w, value, preferred_element_type=jnp.float32)
        total = part if total is None else total + part
    return (total[:, :HEAD_SIZE] / total[:, HEAD_SIZE:]).astype(jnp.bfloat16)


SIDE = 4
CORES = 2
CHIP_SLOTS = SIDE * SIDE
DEVICE_X = SIDE * CORES
UNITS = 2 * KEY_VALUE_HEADS

WAYS = ((1, 0), (-1, 0), (0, 1), (0, -1))
FULL = (
    ((0, 0), None, None),
    ((1, 0), 0, 0),
    ((0, 1), 0, 2),
    ((2, 0), 1, 0),
    ((0, 2), 2, 2),
    ((2, 3), 3, 3),
)
LEAF = (
    ((0, 3), 0, 3),
    ((3, 0), 0, 1),
    ((1, 1), 1, 2),
    ((3, 1), 2, 1),
    ((2, 1), 3, 2),
    ((3, 2), 4, 1),
    ((1, 2), 4, 0),
    ((2, 2), 5, 3),
    ((3, 3), 5, 0),
    ((1, 3), 5, 1),
)
LEAVES = len(LEAF)
PLACES = len(FULL)
ASKERS = 2 * len(WAYS) + 2
PARTNER, SELF = ASKERS - 2, ASKERS - 1
REG_STEPS = 6


def layer_kernel(q_hbm, k_hbm, v_hbm, lists, counts, image, owner, out_hbm, *scratch):
    full_refs = [scratch[u * PLACES : (u + 1) * PLACES] for u in range(UNITS)]
    scratch = scratch[UNITS * PLACES :]
    received = scratch[:UNITS]
    regs_pair = scratch[UNITS : UNITS + REG_STEPS - 1]
    scratch = scratch[REG_STEPS - 1 :]
    (
        outgoing,
        asks,
        asks_s,
        marks,
        regs_in,
        regs,
        q_here,
        out_here,
        weights_here,
        table_sem,
        load_sem,
        regs_sem,
        q_sem,
        out_sem,
        ask_send,
        ask_recv,
        reg_send,
        reg_recv,
        full_send,
        full_recv,
        leaf_send,
        leaf_recv,
        pair_send,
        pair_recv,
    ) = scratch[UNITS:]
    samp = lax.axis_index("samp")
    me = lax.axis_index("seq")
    x = me // DEVICE_X
    y = (me // CORES) % SIDE
    k = me % CORES
    sign = 1 - 2 * k
    blocks, slots = lists.shape
    rows = q_hbm.shape[0] // blocks
    width = GROUP * HEAD_SIZE

    def device(px, py, core):
        return px * DEVICE_X + py * CORES + core

    partner = device(x, y, 1 - k)

    def beside(way, turn, core):
        dx, dy = WAYS[way]
        return device((x + turn * dx + SIDE) % SIDE, (y + turn * dy + SIDE) % SIDE, core)

    def slot(core, offset):
        return core * CHIP_SLOTS + offset[0] * SIDE + offset[1]

    def flag(b, t):
        return jnp.minimum(jnp.maximum(counts[b] - t, 0), 1)

    def remote(src, dst, send_sem, recv_sem, target):
        return pltpu.make_async_remote_copy(
            src_ref=src,
            dst_ref=dst,
            send_sem=send_sem,
            recv_sem=recv_sem,
            device_id=(samp, target),
            device_id_type=pl.DeviceIdType.MESH,
        )

    def load(u):
        hbm = (k_hbm, v_hbm)[u % 2]
        cols = pl.ds((u // 2) * HEAD_SIZE, HEAD_SIZE)
        return pltpu.make_async_copy(hbm.at[:, :, cols], full_refs[u][0], load_sem.at[u])

    def load_regs(c):
        hbm = (k_hbm, v_hbm)[c]
        return pltpu.make_async_copy(
            hbm.at[0, pl.ds(0, REG)], regs_in.at[c], regs_sem.at[c]
        )

    def load_q(h):
        cols = pl.ds(h * width, width)
        return pltpu.make_async_copy(q_hbm.at[:, cols], q_here.at[:, cols], q_sem.at[h])

    def full(u, f):
        _, before, way = FULL[f]
        return remote(
            full_refs[u][before],
            full_refs[u][f],
            full_send.at[u, f],
            full_recv.at[u, f],
            beside(way, sign, k),
        )

    def leaf(u, i, core):
        offset, _, way = LEAF[i]
        return remote(
            outgoing.at[u, 2 * i + core],
            received[u].at[slot(k, offset)],
            leaf_send.at[u, 2 * i + core],
            leaf_recv.at[u, k * LEAVES + i],
            beside(way, sign, core),
        )

    def across(u, f):
        return remote(
            outgoing.at[u, 2 * LEAVES + f],
            received[u].at[slot(k, FULL[f][0])],
            pair_send.at[u, f],
            pair_recv.at[u, f],
            partner,
        )

    def ask(i):
        if i == PARTNER:
            target, there = partner, PARTNER
        else:
            way, core = i // 2, i % 2
            target, there = beside(way, 1, core), 2 * (way ^ 1) + k
        return remote(
            asks.at[SELF], asks.at[there], ask_send.at[i], ask_recv.at[there], target
        )

    load(0).start()
    load(1).start()
    for c in range(2):
        load_regs(c).start()
    for u in range(2, UNITS):
        load(u).start()
    for h in range(KEY_VALUE_HEADS):
        load_q(h).start()

    marks[0] = jnp.zeros((rows, HEAD_SIZE), jnp.bfloat16)
    marks[1] = jnp.ones((rows, HEAD_SIZE), jnp.bfloat16)
    lanes = lax.broadcasted_iota(jnp.int32, (1, 128), 1)
    wanted = jnp.zeros((1, 128), jnp.int32)
    for b in range(blocks):
        for t in range(slots):
            entry = lists[b, t]
            used = flag(b, t)
            wanted = jnp.where(lanes == (entry >> 2) * used + used - 1, entry & 3, wanted)
    asks[SELF] = wanted

    barrier = pltpu.get_barrier_semaphore()
    greeted = [partner] + [beside(way, 1, core) for way in range(4) for core in range(CORES)]
    for target in greeted:
        pl.semaphore_signal(
            barrier, inc=1, device_id=(samp, target), device_id_type=pl.DeviceIdType.MESH
        )
    pl.semaphore_wait(barrier, len(greeted))

    for i in range(PARTNER + 1):
        ask(i).start()

    root = owner[0]
    sides = (
        (root ^ k) & 1,
        ((root >> 3) ^ x) & 1,
        ((root >> 4) ^ (x // 2)) & 1,
        ((root >> 1) ^ y) & 1,
        ((root >> 2) ^ (y // 2)) & 1,
    )
    reg_targets = (
        partner,
        device(x + 1 - 2 * (x % 2), y, k),
        device(SIDE - 1 - x, y, k),
        device(x, y + 1 - 2 * (y % 2), k),
        device(x, SIDE - 1 - y, k),
        partner,
    )

    def reg_copy(i):
        if i == 0:
            src, dst = regs_in.at[1 - k], regs_pair[0].at[1]
        elif i < 5:
            src, dst = regs_pair[i].at[0], regs_pair[i].at[1]
        else:
            src, dst = regs.at[k], regs.at[k]
        return remote(src, dst, reg_send.at[i], reg_recv.at[i], reg_targets[i])

    def reg_step(i):
        if i == 0:
            for c in range(2):
                load_regs(c).wait()
            regs_pair[0][0] = regs_in[k]
        else:
            reg_copy(i - 1).wait_recv()
            chosen = pair_of(i - 1)
            if i < 5:
                regs_pair[i][0] = chosen
            else:
                regs[k] = chosen
        reg_copy(i).start()

    def pair_of(i):
        return regs_pair[i][sides[i]]

    def regs_here():
        remote(
            regs.at[1 - k], regs.at[1 - k], reg_send.at[5], reg_recv.at[5], partner
        ).wait_recv()

    def give(u, f):
        ref = full_refs[u][f]
        offset = FULL[f][0]
        spot = device(
            (x - sign * offset[0] + SIDE) % SIDE, (y - sign * offset[1] + SIDE) % SIDE, k
        )
        for i, (_, before, way) in enumerate(LEAF):
            if before == f:
                turned = way + k if way % 2 == 0 else way - k
                for core in range(CORES):
                    outgoing[u, 2 * i + core] = ref[asks_s[2 * turned + core, 0, spot]]
        outgoing[u, 2 * LEAVES + f] = ref[asks_s[PARTNER, 0, spot]]
        if f:
            received[u][slot(k, offset)] = ref[asks_s[SELF, 0, spot]]
        for i, (_, before, _) in enumerate(LEAF):
            if before == f:
                for core in range(CORES):
                    leaf(u, i, core).start()
        across(u, f).start()

    def begin(u):
        load(u).wait()
        full(u, 1).start()
        full(u, 2).start()

    def stage(u, n):
        if not 0 <= u < UNITS:
            return
        if n == 0:
            give(u, 0)
        elif n == 1:
            for f in (1, 2):
                full(u, f).wait_recv()
                full(u, f + 2).start()
            give(u, 1)
            give(u, 2)
        elif n == 2:
            full(u, 3).wait_recv()
            full(u, 5).start()
            full(u, 4).wait_recv()
            give(u, 3)
            give(u, 4)
        else:
            full(u, 5).wait_recv()
            give(u, 5)

    def all_here(u):
        h = u // 2
        for core in range(CORES):
            for i in range(LEAVES):
                ref = received[u].at[slot(core, LEAF[i][0])]
                remote(
                    ref, ref, leaf_send.at[u, 0], leaf_recv.at[u, core * LEAVES + i], partner
                ).wait_recv()
        for f in range(PLACES):
            ref = received[u].at[slot(1 - k, FULL[f][0])]
            remote(ref, ref, pair_send.at[u, f], pair_recv.at[u, f], partner).wait_recv()
        if u % 2 == 0:
            load_q(h).wait()
            spare = regs[0, :, pl.ds(h * HEAD_SIZE, HEAD_SIZE)]
            received[u][slot(k, (0, 0))] = jnp.concatenate([spare, spare], axis=0)
        else:
            received[u][slot(k, (0, 0))] = jnp.zeros((rows, HEAD_SIZE), jnp.bfloat16)

    def store(h, b):
        return pltpu.make_async_copy(
            out_here.at[h * blocks + b],
            out_hbm.at[pl.ds(pl.multiple_of(b * rows, rows), rows), pl.ds(h * width, width)],
            out_sem.at[h * blocks + b],
        )

    def far_slots(b):
        places = []
        for t in range(slots):
            o = lists[b, t] >> 2
            used = flag(b, t)
            core = o & 1
            turn = 1 - 2 * core
            dx = ((x - (o >> 3)) * turn) & 3
            dy = ((y - (o >> 1)) * turn) & 3
            place = core * CHIP_SLOTS + dx * SIDE + dy
            places.append((place * used + slot(k, (0, 0)) * (1 - used), used))
        return places

    def keys_of(h, b, places):
        return key_pairs(
            full_refs[2 * h][0][b],
            regs[0, :, pl.ds(h * HEAD_SIZE, HEAD_SIZE)],
            [received[2 * h][place] for place, _ in places],
        )

    def values_of(h, b, places):
        return value_pairs(
            full_refs[2 * h + 1][0][b],
            regs[1, :, pl.ds(h * HEAD_SIZE, HEAD_SIZE)],
            [received[2 * h + 1][place] for place, _ in places],
            [marks[used] for _, used in places],
        )

    def queries_of(h, b):
        here = pl.ds(pl.multiple_of(b * rows, rows), rows)
        return stacked_heads(q_here[here, pl.ds(h * width, width)])

    part = rows * GROUP // PARTS

    def compute(h, start, stop):
        @pl.loop(start, stop)
        def _(b):
            places = far_slots(b)
            stacked = queries_of(h, b)
            keys, values = keys_of(h, b, places), values_of(h, b, places)
            seen = seen_rows(rows, image[b])
            scores = [score(stacked, keys, seen, 0, part)]
            outs = []
            for n in range(PARTS):
                if n + 1 < PARTS:
                    scores.append(
                        score(stacked, keys, seen, (n + 1) * part, (n + 2) * part)
                    )
                outs.append(finish(soften(scores[n]), values))
            out_here[h * blocks + b] = spread_heads(jnp.concatenate(outs, axis=0), rows)
            store(h, b).start()

    def compute_weights(h):
        @pl.loop(0, blocks)
        def _(b):
            stacked = queries_of(h, b)
            keys = keys_of(h, b, far_slots(b))
            seen = seen_rows(rows, image[b])
            scores = [score(stacked, keys, seen, 0, part)]
            for n in range(PARTS):
                if n + 1 < PARTS:
                    scores.append(
                        score(stacked, keys, seen, (n + 1) * part, (n + 2) * part)
                    )
                for i, w in enumerate(soften(scores[n])):
                    weights_here[b, i, pl.ds(n * part, part)] = w

    def compute_outputs(h):
        @pl.loop(0, blocks)
        def _(b):
            values = values_of(h, b, far_slots(b))
            pairs = len(values)
            outs = finish([weights_here[b, i] for i in range(pairs)], values)
            out_here[h * blocks + b] = spread_heads(outs, rows)
            store(h, b).start()

    begin(0)
    begin(1)
    reg_step(0)
    begin(2)
    for i in range(PARTNER + 1):
        ref = asks.at[i]
        remote(ref, ref, ask_send.at[i], ask_recv.at[i], partner).wait_recv()
    to_scalars = pltpu.make_async_copy(asks, asks_s, table_sem.at[0])
    to_scalars.start()
    to_scalars.wait()
    stage(0, 0)
    stage(1, 0)
    reg_step(1)
    stage(2, 0)
    last = KEY_VALUE_HEADS - 1
    half = blocks // 2
    for t in range(UNITS + 2):
        stage(t, 1)
        stage(t - 1, 2)
        stage(t - 2, 3)
        if t + 3 < UNITS:
            begin(t + 3)
            stage(t + 3, 0)
        if t + 2 < REG_STEPS:
            reg_step(t + 2)
        if t == REG_STEPS - 2:
            regs_here()
        if t >= 4:
            h = t // 2 - 2
            if t % 2 == 0:
                all_here(2 * h)
                all_here(2 * h + 1)
                compute(h, 0, half)
            else:
                compute(h, half, blocks)
    all_here(2 * last)
    compute_weights(last)
    all_here(2 * last + 1)
    compute_outputs(last)

    for i in range(PARTNER + 1):
        ask(i).wait_send()
    for i in range(REG_STEPS):
        reg_copy(i).wait_send()
    for u in range(UNITS):
        for f in range(1, PLACES):
            full(u, f).wait_send()
        for f in range(PLACES):
            across(u, f).wait_send()
        for i in range(LEAVES):
            for core in range(CORES):
                leaf(u, i, core).wait_send()
    for h in range(KEY_VALUE_HEADS):
        for b in range(blocks):
            store(h, b).wait()


def layer(q, k, v, lists, counts, image, owner):
    blocks, slots = lists.shape
    rows = q.shape[0] // blocks
    kv_width = k.shape[1]
    width = GROUP * HEAD_SIZE
    heads = KEY_VALUE_HEADS
    bf16 = jnp.bfloat16
    dma = pltpu.SemaphoreType.DMA
    return pl.pallas_call(
        layer_kernel,
        out_shape=jax.ShapeDtypeStruct(q.shape, bf16),
        in_specs=[pl.BlockSpec(memory_space=pl.ANY)] * 3
        + [pl.BlockSpec(memory_space=pltpu.SMEM)] * 4,
        out_specs=pl.BlockSpec(memory_space=pl.ANY),
        scratch_shapes=[pltpu.VMEM((blocks, rows, HEAD_SIZE), bf16)] * (UNITS * PLACES)
        + [pltpu.VMEM((CORES * CHIP_SLOTS, rows, HEAD_SIZE), bf16)] * UNITS
        + [pltpu.VMEM((2, REG, kv_width), bf16)] * (REG_STEPS - 1)
        + [
            pltpu.VMEM((UNITS, 2 * LEAVES + PLACES, rows, HEAD_SIZE), bf16),
            pltpu.VMEM((ASKERS, 1, 128), jnp.int32),
            pltpu.SMEM((ASKERS, 1, 128), jnp.int32),
            pltpu.VMEM((2, rows, HEAD_SIZE), bf16),
            pltpu.VMEM((2, REG, kv_width), bf16),
            pltpu.VMEM((2, REG, kv_width), bf16),
            pltpu.VMEM(q.shape, bf16),
            pltpu.VMEM((heads * blocks, rows, width), bf16),
            pltpu.VMEM((blocks, (slots + 2) // 2, GROUP * rows, 2 * rows), bf16),
            dma((1,)),
            dma((UNITS,)),
            dma((2,)),
            dma((heads,)),
            dma((heads * blocks,)),
            dma((PARTNER + 1,)),
            dma((PARTNER + 1,)),
            dma((REG_STEPS,)),
            dma((REG_STEPS,)),
            dma((UNITS, PLACES)),
            dma((UNITS, PLACES)),
            dma((UNITS, 2 * LEAVES)),
            dma((UNITS, 2 * LEAVES)),
            dma((UNITS, PLACES)),
            dma((UNITS, PLACES)),
        ],
        compiler_params=pltpu.CompilerParams(
            collective_id=0, has_side_effects=True, vmem_limit_bytes=62 << 20
        ),
        name="layer",
    )(
        q,
        k.reshape(blocks, rows, kv_width),
        v.reshape(blocks, rows, kv_width),
        lists,
        counts,
        image,
        owner,
    )


def per_device(queries, keys, values, reg_owner, block_lists, list_counts, image_blocks):
    out = layer(
        queries[0],
        keys[0],
        values[0],
        block_lists[0],
        list_counts[0],
        image_blocks[0],
        reg_owner,
    )
    return out[None]


def solution(mesh):
    placed = (
        P("samp", "seq", None),
        P("samp", "seq", None),
        P("samp", "seq", None),
        P("samp"),
        P("samp", "seq", None),
        P("samp", "seq"),
        P("samp", "seq"),
    )
    return jax.shard_map(
        per_device, mesh=mesh, in_specs=placed, out_specs=P("samp", "seq", None), check_vma=False
    )
```

```python
import math

import jax
import jax.numpy as jnp
from jax import lax
from jax.experimental import pallas as pl
from jax.experimental.pallas import tpu as pltpu
from jax.sharding import PartitionSpec as P

QUERY_HEADS = 28
KEY_VALUE_HEADS = 4
HEAD_SIZE = 128
REG = 64
GROUP = QUERY_HEADS // KEY_VALUE_HEADS
SCALE = math.log2(math.e) / math.sqrt(HEAD_SIZE)


very_low = -1e30


def dot_t(a, b):
    return lax.dot_general(a, b, (((1,), (1,)), ((), ())), preferred_element_type=jnp.float32)


PARTS = 4


def stacked_heads(q):
    return jnp.concatenate(
        [q[:, g * HEAD_SIZE : (g + 1) * HEAD_SIZE] for g in range(GROUP)], axis=0
    )


def spread_heads(merged, rows):
    return jnp.concatenate([merged[g * rows : (g + 1) * rows] for g in range(GROUP)], axis=1)


def paired(blocks):
    return [
        jnp.concatenate([blocks[i], blocks[i + 1]], axis=0) for i in range(0, len(blocks), 2)
    ]


def key_pairs(own_k, reg_k, far):
    return paired([own_k, jnp.concatenate([reg_k, reg_k], axis=0)] + far)


def value_pairs(own_v, reg_v, far, used):
    rows = own_v.shape[0]
    zero = jnp.zeros((rows, HEAD_SIZE), jnp.bfloat16)
    ones = jnp.ones((rows, HEAD_SIZE), jnp.bfloat16)
    half = jnp.concatenate([ones[:REG], zero[:REG]], axis=0)
    values = [own_v, jnp.concatenate([reg_v, zero[:REG]], axis=0)] + far
    marks = [ones, half] + used
    return paired([jnp.concatenate([v, m], axis=1) for v, m in zip(values, marks)])


def seen_rows(rows, is_image):
    visible = lax.broadcasted_iota(jnp.int32, (rows, rows), 1) <= (
        lax.broadcasted_iota(jnp.int32, (rows, rows), 0) + is_image * rows
    )
    return jnp.concatenate([visible] * GROUP, axis=0)


def score(stacked, keys, seen, lo, hi):
    rows = seen.shape[1]
    scores = [dot_t(stacked[lo:hi], key) for key in keys]
    own = jnp.where(seen[lo:hi], scores[0][:, :rows], very_low)
    scores[0] = jnp.concatenate([own, scores[0][:, rows:]], axis=1)
    return scores


def soften(scores):
    top = scores[0]
    for s in scores[1:]:
        top = jnp.maximum(top, s)
    top = jnp.max(top, axis=1, keepdims=True)
    return [jnp.exp2((s - top) * SCALE).astype(jnp.bfloat16) for s in scores]


def finish(weights, values):
    total = None
    for w, value in zip(weights, values):
        part = jnp.dot(w, value, preferred_element_type=jnp.float32)
        total = part if total is None else total + part
    return (total[:, :HEAD_SIZE] / total[:, HEAD_SIZE:]).astype(jnp.bfloat16)


SIDE = 4
CORES = 2
CHIP_SLOTS = SIDE * SIDE
DEVICE_X = SIDE * CORES
ORDER = ((0, 0), (0, 1), (1, 0), (1, 1), (2, 0), (3, 0), (2, 1), (3, 1))
UNITS = len(ORDER)
KEYS = {h: u for u, (h, c) in enumerate(ORDER) if c == 0}
VALUES = {h: u for u, (h, c) in enumerate(ORDER) if c == 1}
LEAD = 2

WAYS = ((1, 0), (-1, 0), (0, 1), (0, -1))
FULL = (
    ((0, 0), None, None),
    ((1, 0), 0, 0),
    ((0, 1), 0, 2),
    ((2, 0), 1, 0),
    ((0, 2), 2, 2),
    ((2, 3), 3, 3),
)
LEAF = (
    ((0, 3), 0, 3),
    ((3, 0), 0, 1),
    ((1, 1), 1, 2),
    ((3, 1), 2, 1),
    ((2, 1), 3, 2),
    ((3, 2), 4, 1),
    ((1, 2), 4, 0),
    ((2, 2), 5, 3),
    ((3, 3), 5, 0),
    ((1, 3), 5, 1),
)
LEAVES = len(LEAF)
PLACES = len(FULL)
MESSAGES = 2 * LEAVES + PLACES
ASKERS = 2 * len(WAYS) + 2
PARTNER, SELF = ASKERS - 2, ASKERS - 1
REG_STEPS = 5
REG_COPIES = REG_STEPS + 2


def layer_kernel(
    q_hbm, k_hbm, v_hbm, lists_hbm, counts_hbm, image_hbm, owner_hbm, out_hbm, *scratch
):
    lists, counts, image, owner, small_sem = scratch[:5]
    scratch = scratch[5:]
    full_refs = [scratch[u * PLACES : (u + 1) * PLACES] for u in range(UNITS)]
    scratch = scratch[UNITS * PLACES :]
    received = scratch[:UNITS]
    regs_pair = scratch[UNITS : UNITS + REG_STEPS - 1]
    scratch = scratch[REG_STEPS - 1 :]
    (
        outgoing,
        asks,
        asks_s,
        marks,
        regs_in,
        regs,
        q_here,
        out_here,
        weights_here,
        table_sem,
        load_sem,
        regs_sem,
        q_sem,
        out_sem,
        ask_send,
        ask_recv,
        reg_send,
        reg_recv,
        full_send,
        full_recv,
        unit_send,
        unit_recv,
    ) = scratch[UNITS:]
    samp = lax.axis_index("samp")
    me = lax.axis_index("seq")
    x = me // DEVICE_X
    y = (me // CORES) % SIDE
    k = me % CORES
    sign = 1 - 2 * k
    blocks, slots = lists.shape
    rows = q_hbm.shape[0] // blocks
    width = GROUP * HEAD_SIZE

    def device(px, py, core):
        return px * DEVICE_X + py * CORES + core

    partner = device(x, y, 1 - k)

    def beside(way, turn, core):
        dx, dy = WAYS[way]
        return device((x + turn * dx + SIDE) % SIDE, (y + turn * dy + SIDE) % SIDE, core)

    def slot(core, offset):
        return core * CHIP_SLOTS + offset[0] * SIDE + offset[1]

    def flag(b, t):
        return jnp.minimum(jnp.maximum(counts[b] - t, 0), 1)

    def remote(src, dst, send_sem, recv_sem, target):
        return pltpu.make_async_remote_copy(
            src_ref=src,
            dst_ref=dst,
            send_sem=send_sem,
            recv_sem=recv_sem,
            device_id=(samp, target),
            device_id_type=pl.DeviceIdType.MESH,
        )

    def load(u):
        h, c = ORDER[u]
        hbm = (k_hbm, v_hbm)[c]
        cols = pl.ds(h * HEAD_SIZE, HEAD_SIZE)
        return pltpu.make_async_copy(hbm.at[:, :, cols], full_refs[u][0], load_sem.at[u])

    def load_regs(c):
        hbm = (k_hbm, v_hbm)[c]
        return pltpu.make_async_copy(
            hbm.at[0, pl.ds(0, REG)], regs_in.at[c], regs_sem.at[c]
        )

    def load_q(h):
        cols = pl.ds(h * width, width)
        return pltpu.make_async_copy(q_hbm.at[:, cols], q_here.at[:, cols], q_sem.at[h])

    def full(u, f):
        _, before, way = FULL[f]
        return remote(
            full_refs[u][before],
            full_refs[u][f],
            full_send.at[u],
            full_recv.at[u, f],
            beside(way, sign, k),
        )

    def leaf(u, i, core):
        offset, _, way = LEAF[i]
        return remote(
            outgoing.at[u, 2 * i + core],
            received[u].at[slot(k, offset)],
            unit_send.at[u],
            unit_recv.at[u],
            beside(way, sign, core),
        )

    def across(u, f):
        return remote(
            outgoing.at[u, 2 * LEAVES + f],
            received[u].at[slot(k, FULL[f][0])],
            unit_send.at[u],
            unit_recv.at[u],
            partner,
        )

    def ask(i):
        if i == PARTNER:
            target, there = partner, PARTNER
        else:
            way, core = i // 2, i % 2
            target, there = beside(way, 1, core), 2 * (way ^ 1) + k
        return remote(
            asks.at[SELF], asks.at[there], ask_send.at[0], ask_recv.at[0], target
        )

    barrier = pltpu.get_barrier_semaphore()
    greeted = [partner] + [beside(way, 1, core) for way in range(4) for core in range(CORES)]
    for target in greeted:
        pl.semaphore_signal(
            barrier, inc=1, device_id=(samp, target), device_id_type=pl.DeviceIdType.MESH
        )
    small = [
        pltpu.make_async_copy(src, dst, small_sem.at[i])
        for i, (src, dst) in enumerate(
            (
                (lists_hbm, lists),
                (counts_hbm, counts),
                (image_hbm, image),
                (owner_hbm, owner),
            )
        )
    ]
    for copy in small:
        copy.start()
    for c in range(2):
        load_regs(c).start()
    load(0).start()
    load(1).start()
    for u in range(2, UNITS):
        load(u).start()
    for h in range(KEY_VALUE_HEADS):
        load_q(h).start()

    marks[0] = jnp.zeros((rows, HEAD_SIZE), jnp.bfloat16)
    marks[1] = jnp.ones((rows, HEAD_SIZE), jnp.bfloat16)
    for copy in small:
        copy.wait()
    lanes = lax.broadcasted_iota(jnp.int32, (1, 128), 1)
    wanted = jnp.zeros((1, 128), jnp.int32)
    for b in range(blocks):
        for t in range(slots):
            entry = lists[b, t]
            used = flag(b, t)
            wanted = jnp.where(lanes == (entry >> 2) * used + used - 1, entry & 3, wanted)
    asks[SELF] = wanted

    pl.semaphore_wait(barrier, len(greeted))

    for i in range(PARTNER + 1):
        ask(i).start()

    root = owner[0]
    sides = (
        (((root >> 3) ^ x) & 1) * 2 + ((root ^ k) & 1),
        ((root >> 4) ^ (x // 2)) & 1,
        ((root >> 1) ^ y) & 1,
        ((root >> 2) ^ (y // 2)) & 1,
    )
    opposite = x + 1 - 2 * (x % 2)
    reg_targets = (
        partner,
        device(opposite, y, k),
        device(opposite, y, 1 - k),
        device(SIDE - 1 - x, y, k),
        device(x, y + 1 - 2 * (y % 2), k),
        device(x, SIDE - 1 - y, k),
        partner,
    )

    def reg_copy(i):
        if i < 3:
            src, dst = regs_in.at[k if i == 1 else 1 - k], regs_pair[0].at[i + 1]
        elif i < REG_COPIES - 1:
            src, dst = regs_pair[i - 2].at[0], regs_pair[i - 2].at[1]
        else:
            src, dst = regs.at[k], regs.at[k]
        return remote(src, dst, reg_send.at[i], reg_recv.at[i], reg_targets[i])

    def reg_step(i):
        if i == 0:
            for c in range(2):
                load_regs(c).wait()
            for n in range(3):
                reg_copy(n).start()
            regs_pair[0][0] = regs_in[k]
            return
        for n in range(3) if i == 1 else (i + 1,):
            reg_copy(n).wait_recv()
        chosen = regs_pair[i - 1][sides[i - 1]]
        if i < REG_STEPS - 1:
            regs_pair[i][0] = chosen
        else:
            regs[k] = chosen
        reg_copy(i + 2).start()

    def regs_here():
        remote(
            regs.at[1 - k], regs.at[1 - k], reg_send.at[REG_COPIES - 1], reg_recv.at[REG_COPIES - 1], partner
        ).wait_recv()

    def give(u, f):
        ref = full_refs[u][f]
        offset = FULL[f][0]
        spot = device(
            (x - sign * offset[0] + SIDE) % SIDE, (y - sign * offset[1] + SIDE) % SIDE, k
        )
        for i, (_, before, way) in enumerate(LEAF):
            if before == f:
                turned = way + k if way % 2 == 0 else way - k
                for core in range(CORES):
                    outgoing[u, 2 * i + core] = ref[asks_s[2 * turned + core, 0, spot]]
        outgoing[u, 2 * LEAVES + f] = ref[asks_s[PARTNER, 0, spot]]
        if f:
            received[u][slot(k, offset)] = ref[asks_s[SELF, 0, spot]]
        for i, (_, before, _) in enumerate(LEAF):
            if before == f:
                for core in range(CORES):
                    leaf(u, i, core).start()
        across(u, f).start()

    def begin(u):
        load(u).wait()
        full(u, 1).start()
        full(u, 2).start()

    def stage(u, n):
        if not 0 <= u < UNITS:
            return
        if n == 0:
            give(u, 0)
        elif n == 1:
            for f in (1, 2):
                full(u, f).wait_recv()
                full(u, f + 2).start()
            give(u, 1)
            give(u, 2)
        elif n == 2:
            full(u, 3).wait_recv()
            full(u, 5).start()
            full(u, 4).wait_recv()
            give(u, 3)
            give(u, 4)
        else:
            full(u, 5).wait_recv()
            give(u, 5)

    def all_here(u):
        h, c = ORDER[u]
        ref = received[u].at[pl.ds(0, MESSAGES)]
        remote(ref, ref, unit_send.at[u], unit_recv.at[u], partner).wait_recv()
        if c == 0:
            load_q(h).wait()
            spare = regs[0, :, pl.ds(h * HEAD_SIZE, HEAD_SIZE)]
            received[u][slot(k, (0, 0))] = jnp.concatenate([spare, spare], axis=0)
        else:
            received[u][slot(k, (0, 0))] = jnp.zeros((rows, HEAD_SIZE), jnp.bfloat16)

    def store(h, b):
        return pltpu.make_async_copy(
            out_here.at[h * blocks + b],
            out_hbm.at[pl.ds(pl.multiple_of(b * rows, rows), rows), pl.ds(h * width, width)],
            out_sem.at[h * blocks + b],
        )

    def far_slots(b):
        places = []
        for t in range(slots):
            o = lists[b, t] >> 2
            used = flag(b, t)
            core = o & 1
            turn = 1 - 2 * core
            dx = ((x - (o >> 3)) * turn) & 3
            dy = ((y - (o >> 1)) * turn) & 3
            place = core * CHIP_SLOTS + dx * SIDE + dy
            places.append((place * used + slot(k, (0, 0)) * (1 - used), used))
        return places

    def keys_of(h, b, places):
        return key_pairs(
            full_refs[KEYS[h]][0][b],
            regs[0, :, pl.ds(h * HEAD_SIZE, HEAD_SIZE)],
            [received[KEYS[h]][place] for place, _ in places],
        )

    def values_of(h, b, places):
        return value_pairs(
            full_refs[VALUES[h]][0][b],
            regs[1, :, pl.ds(h * HEAD_SIZE, HEAD_SIZE)],
            [received[VALUES[h]][place] for place, _ in places],
            [marks[used] for _, used in places],
        )

    def queries_of(h, b):
        here = pl.ds(pl.multiple_of(b * rows, rows), rows)
        return stacked_heads(q_here[here, pl.ds(h * width, width)])

    part = rows * GROUP // PARTS

    def compute_weights(h):
        @pl.loop(0, blocks)
        def _(b):
            stacked = queries_of(h, b)
            keys = keys_of(h, b, far_slots(b))
            seen = seen_rows(rows, image[b])
            scores = [score(stacked, keys, seen, 0, part)]
            for n in range(PARTS):
                if n + 1 < PARTS:
                    scores.append(
                        score(stacked, keys, seen, (n + 1) * part, (n + 2) * part)
                    )
                for i, w in enumerate(soften(scores[n])):
                    weights_here[h % 2, b, i, pl.ds(n * part, part)] = w

    def compute_outputs(h):
        @pl.loop(0, blocks)
        def _(b):
            values = values_of(h, b, far_slots(b))
            pairs = len(values)
            outs = finish([weights_here[h % 2, b, i] for i in range(pairs)], values)
            out_here[h * blocks + b] = spread_heads(outs, rows)
            store(h, b).start()

    reg_step(0)
    for u in range(LEAD):
        begin(u)
    others = asks.at[pl.ds(0, SELF)]
    remote(others, others, ask_send.at[0], ask_recv.at[0], partner).wait_recv()
    to_scalars = pltpu.make_async_copy(asks, asks_s, table_sem.at[0])
    to_scalars.start()
    to_scalars.wait()
    stage(0, 0)
    reg_step(1)
    for u in range(1, LEAD):
        stage(u, 0)
    for t in range(UNITS + 3):
        stage(t, 1)
        stage(t - 1, 2)
        stage(t - 2, 3)
        if t + LEAD < UNITS:
            begin(t + LEAD)
            stage(t + LEAD, 0)
        if t + 2 < REG_STEPS:
            reg_step(t + 2)
        elif t + 2 == REG_STEPS:
            regs_here()
        if t >= 3:
            h, c = ORDER[t - 3]
            all_here(t - 3)
            if c == 0:
                compute_weights(h)
            else:
                compute_outputs(h)

    remote(others, others, ask_send.at[0], ask_recv.at[0], partner).wait_send()
    for i in range(REG_COPIES):
        reg_copy(i).wait_send()
    for u in range(UNITS):
        sent = outgoing.at[u]
        remote(sent, sent, unit_send.at[u], unit_recv.at[u], partner).wait_send()
        sent = outgoing.at[u, pl.ds(0, (PLACES - 1) * blocks)]
        remote(sent, sent, full_send.at[u], unit_recv.at[u], partner).wait_send()
    for h in range(KEY_VALUE_HEADS):
        for b in range(blocks):
            store(h, b).wait()


def layer(q, k, v, lists, counts, image, owner):
    blocks, slots = lists.shape
    rows = q.shape[0] // blocks
    kv_width = k.shape[1]
    width = GROUP * HEAD_SIZE
    heads = KEY_VALUE_HEADS
    bf16 = jnp.bfloat16
    dma = pltpu.SemaphoreType.DMA
    return pl.pallas_call(
        layer_kernel,
        out_shape=jax.ShapeDtypeStruct(q.shape, bf16),
        in_specs=[pl.BlockSpec(memory_space=pl.ANY)] * 7,
        out_specs=pl.BlockSpec(memory_space=pl.ANY),
        scratch_shapes=[pltpu.SMEM(a.shape, jnp.int32) for a in (lists, counts, image, owner)]
        + [dma((4,))]
        + [pltpu.VMEM((blocks, rows, HEAD_SIZE), bf16)] * (UNITS * PLACES)
        + [pltpu.VMEM((CORES * CHIP_SLOTS, rows, HEAD_SIZE), bf16)] * UNITS
        + [pltpu.VMEM((4, REG, kv_width), bf16)]
        + [pltpu.VMEM((2, REG, kv_width), bf16)] * (REG_STEPS - 2)
        + [
            pltpu.VMEM((UNITS, 2 * LEAVES + PLACES, rows, HEAD_SIZE), bf16),
            pltpu.VMEM((ASKERS, 1, 128), jnp.int32),
            pltpu.SMEM((ASKERS, 1, 128), jnp.int32),
            pltpu.VMEM((2, rows, HEAD_SIZE), bf16),
            pltpu.VMEM((2, REG, kv_width), bf16),
            pltpu.VMEM((2, REG, kv_width), bf16),
            pltpu.VMEM(q.shape, bf16),
            pltpu.VMEM((heads * blocks, rows, width), bf16),
            pltpu.VMEM((2, blocks, (slots + 2) // 2, GROUP * rows, 2 * rows), bf16),
            dma((1,)),
            dma((UNITS,)),
            dma((2,)),
            dma((heads,)),
            dma((heads * blocks,)),
            dma((1,)),
            dma((1,)),
            dma((REG_COPIES,)),
            dma((REG_COPIES,)),
            dma((UNITS,)),
            dma((UNITS, PLACES)),
            dma((UNITS,)),
            dma((UNITS,)),
        ],
        compiler_params=pltpu.CompilerParams(
            collective_id=0, has_side_effects=True, vmem_limit_bytes=62 << 20
        ),
        name="layer",
    )(
        q,
        k.reshape(blocks, rows, kv_width),
        v.reshape(blocks, rows, kv_width),
        lists,
        counts,
        image,
        owner,
    )


def per_device(queries, keys, values, reg_owner, block_lists, list_counts, image_blocks):
    out = layer(
        queries[0],
        keys[0],
        values[0],
        block_lists[0],
        list_counts[0],
        image_blocks[0],
        reg_owner,
    )
    return out[None]


def solution(mesh):
    placed = (
        P("samp", "seq", None),
        P("samp", "seq", None),
        P("samp", "seq", None),
        P("samp"),
        P("samp", "seq", None),
        P("samp", "seq"),
        P("samp", "seq"),
    )
    return jax.shard_map(
        per_device, mesh=mesh, in_specs=placed, out_specs=P("samp", "seq", None), check_vma=False
    )
```

```python
import math

import jax
import jax.numpy as jnp
from jax import lax
from jax.experimental import pallas as pl
from jax.experimental.pallas import tpu as pltpu
from jax.sharding import PartitionSpec as P

QUERY_HEADS = 28
KEY_VALUE_HEADS = 4
HEAD_SIZE = 128
REG = 64
GROUP = QUERY_HEADS // KEY_VALUE_HEADS
SCALE = math.log2(math.e) / math.sqrt(HEAD_SIZE)


very_low = -1e30


def dot_t(a, b):
    return lax.dot_general(a, b, (((1,), (1,)), ((), ())), preferred_element_type=jnp.float32)


PARTS = 4


def stacked_heads(q):
    return jnp.concatenate(
        [q[:, g * HEAD_SIZE : (g + 1) * HEAD_SIZE] for g in range(GROUP)], axis=0
    )


def spread_heads(merged, rows):
    return jnp.concatenate([merged[g * rows : (g + 1) * rows] for g in range(GROUP)], axis=1)


def paired(blocks):
    return [
        jnp.concatenate([blocks[i], blocks[i + 1]], axis=0) for i in range(0, len(blocks), 2)
    ]


def key_pairs(own_k, reg_k, far):
    return paired([own_k, jnp.concatenate([reg_k, reg_k], axis=0)] + far)


def value_pairs(own_v, reg_v, far, used):
    rows = own_v.shape[0]
    zero = jnp.zeros((rows, HEAD_SIZE), jnp.bfloat16)
    ones = jnp.ones((rows, HEAD_SIZE), jnp.bfloat16)
    half = jnp.concatenate([ones[:REG], zero[:REG]], axis=0)
    values = [own_v, jnp.concatenate([reg_v, zero[:REG]], axis=0)] + far
    marks = [ones, half] + used
    return paired([jnp.concatenate([v, m], axis=1) for v, m in zip(values, marks)])


def seen_rows(rows, is_image):
    visible = lax.broadcasted_iota(jnp.int32, (rows, rows), 1) <= (
        lax.broadcasted_iota(jnp.int32, (rows, rows), 0) + is_image * rows
    )
    return jnp.concatenate([visible] * GROUP, axis=0)


def score(stacked, keys, seen, lo, hi):
    rows = seen.shape[1]
    scores = [dot_t(stacked[lo:hi], key) for key in keys]
    own = jnp.where(seen[lo:hi], scores[0][:, :rows], very_low)
    scores[0] = jnp.concatenate([own, scores[0][:, rows:]], axis=1)
    return scores


def soften(scores):
    top = scores[0]
    for s in scores[1:]:
        top = jnp.maximum(top, s)
    top = jnp.max(top, axis=1, keepdims=True)
    return [jnp.exp2((s - top) * SCALE).astype(jnp.bfloat16) for s in scores]


def finish(weights, values):
    total = None
    for w, value in zip(weights, values):
        part = jnp.dot(w, value, preferred_element_type=jnp.float32)
        total = part if total is None else total + part
    return (total[:, :HEAD_SIZE] / total[:, HEAD_SIZE:]).astype(jnp.bfloat16)


SIDE = 4
CORES = 2
CHIP_SLOTS = SIDE * SIDE
DEVICE_X = SIDE * CORES
ORDER = ((0, 0), (0, 1), (1, 0), (1, 1), (2, 0), (3, 0), (2, 1), (3, 1))
UNITS = len(ORDER)
KEYS = {h: u for u, (h, c) in enumerate(ORDER) if c == 0}
VALUES = {h: u for u, (h, c) in enumerate(ORDER) if c == 1}
LEAD = 2

WAYS = ((1, 0), (-1, 0), (0, 1), (0, -1))
FULL = (
    ((0, 0), None, None),
    ((1, 0), 0, 0),
    ((0, 1), 0, 2),
    ((2, 0), 1, 0),
    ((0, 2), 2, 2),
    ((2, 3), 3, 3),
)
LEAF = (
    ((0, 3), 0, 3),
    ((3, 0), 0, 1),
    ((1, 1), 1, 2),
    ((3, 1), 2, 1),
    ((2, 1), 3, 2),
    ((3, 2), 4, 1),
    ((1, 2), 4, 0),
    ((2, 2), 5, 3),
    ((3, 3), 5, 0),
    ((1, 3), 5, 1),
)
LEAVES = len(LEAF)
PLACES = len(FULL)
MESSAGES = 2 * LEAVES + PLACES
ASKERS = 2 * len(WAYS) + 2
PARTNER, SELF = ASKERS - 2, ASKERS - 1
REG_STEPS = 5
REG_COPIES = REG_STEPS + 2


def layer_kernel(
    q_hbm, k_hbm, v_hbm, lists_hbm, counts_hbm, image_hbm, owner_hbm, out_hbm, *scratch
):
    lists, counts, image, owner, small_sem = scratch[:5]
    scratch = scratch[5:]
    full_refs = [scratch[u * PLACES : (u + 1) * PLACES] for u in range(UNITS)]
    scratch = scratch[UNITS * PLACES :]
    received = scratch[:UNITS]
    regs_pair = scratch[UNITS : UNITS + REG_STEPS - 1]
    scratch = scratch[REG_STEPS - 1 :]
    (
        outgoing,
        asks,
        asks_s,
        marks,
        regs_in,
        regs,
        q_here,
        out_here,
        weights_here,
        table_sem,
        load_sem,
        regs_sem,
        q_sem,
        out_sem,
        ask_send,
        ask_recv,
        reg_send,
        reg_recv,
        full_send,
        full_recv,
        unit_send,
        unit_recv,
    ) = scratch[UNITS:]
    samp = lax.axis_index("samp")
    me = lax.axis_index("seq")
    x = me // DEVICE_X
    y = (me // CORES) % SIDE
    k = me % CORES
    sign = 1 - 2 * k
    blocks, slots = lists.shape
    rows = q_hbm.shape[0] // blocks
    width = GROUP * HEAD_SIZE

    def device(px, py, core):
        return px * DEVICE_X + py * CORES + core

    partner = device(x, y, 1 - k)

    def beside(way, turn, core):
        dx, dy = WAYS[way]
        return device((x + turn * dx + SIDE) % SIDE, (y + turn * dy + SIDE) % SIDE, core)

    def slot(core, offset):
        return core * CHIP_SLOTS + offset[0] * SIDE + offset[1]

    def flag(b, t):
        return jnp.minimum(jnp.maximum(counts[b] - t, 0), 1)

    def remote(src, dst, send_sem, recv_sem, target):
        return pltpu.make_async_remote_copy(
            src_ref=src,
            dst_ref=dst,
            send_sem=send_sem,
            recv_sem=recv_sem,
            device_id=(samp, target),
            device_id_type=pl.DeviceIdType.MESH,
        )

    def load(u):
        h, c = ORDER[u]
        hbm = (k_hbm, v_hbm)[c]
        cols = pl.ds(h * HEAD_SIZE, HEAD_SIZE)
        return pltpu.make_async_copy(hbm.at[:, :, cols], full_refs[u][0], load_sem.at[u])

    def load_regs(c):
        hbm = (k_hbm, v_hbm)[c]
        return pltpu.make_async_copy(
            hbm.at[0, pl.ds(0, REG)], regs_in.at[c], regs_sem.at[c]
        )

    def load_q(h):
        cols = pl.ds(h * width, width)
        return pltpu.make_async_copy(q_hbm.at[:, cols], q_here.at[:, cols], q_sem.at[h])

    def full(u, f):
        _, before, way = FULL[f]
        return remote(
            full_refs[u][before],
            full_refs[u][f],
            full_send.at[u],
            full_recv.at[u, f],
            beside(way, sign, k),
        )

    def leaf(u, i, core):
        offset, _, way = LEAF[i]
        return remote(
            outgoing.at[u, 2 * i + core],
            received[u].at[slot(k, offset)],
            unit_send.at[u],
            unit_recv.at[u],
            beside(way, sign, core),
        )

    def across(u, f):
        return remote(
            outgoing.at[u, 2 * LEAVES + f],
            received[u].at[slot(k, FULL[f][0])],
            unit_send.at[u],
            unit_recv.at[u],
            partner,
        )

    def ask(i):
        if i == PARTNER:
            target, there = partner, PARTNER
        else:
            way, core = i // 2, i % 2
            target, there = beside(way, 1, core), 2 * (way ^ 1) + k
        return remote(
            asks.at[SELF], asks.at[there], ask_send.at[0], ask_recv.at[0], target
        )

    barrier = pltpu.get_barrier_semaphore()
    greeted = [partner] + [beside(way, 1, core) for way in range(4) for core in range(CORES)]
    for target in greeted:
        pl.semaphore_signal(
            barrier, inc=1, device_id=(samp, target), device_id_type=pl.DeviceIdType.MESH
        )
    small = [
        pltpu.make_async_copy(src, dst, small_sem.at[i])
        for i, (src, dst) in enumerate(
            (
                (lists_hbm, lists),
                (counts_hbm, counts),
                (image_hbm, image),
                (owner_hbm, owner),
            )
        )
    ]
    for copy in small:
        copy.start()
    for c in range(2):
        load_regs(c).start()
    load(0).start()
    load(1).start()
    for u in range(2, UNITS):
        load(u).start()
    for h in range(KEY_VALUE_HEADS):
        load_q(h).start()

    marks[0] = jnp.zeros((rows, HEAD_SIZE), jnp.bfloat16)
    marks[1] = jnp.ones((rows, HEAD_SIZE), jnp.bfloat16)
    for copy in small:
        copy.wait()
    lanes = lax.broadcasted_iota(jnp.int32, (1, 128), 1)
    wanted = jnp.zeros((1, 128), jnp.int32)
    for b in range(blocks):
        for t in range(slots):
            entry = lists[b, t]
            used = flag(b, t)
            wanted = jnp.where(lanes == (entry >> 2) * used + used - 1, entry & 3, wanted)
    asks[SELF] = wanted

    pl.semaphore_wait(barrier, len(greeted))

    for i in range(PARTNER + 1):
        ask(i).start()

    root = owner[0]
    sides = (
        (((root >> 3) ^ x) & 1) * 2 + ((root ^ k) & 1),
        ((root >> 4) ^ (x // 2)) & 1,
        ((root >> 1) ^ y) & 1,
        ((root >> 2) ^ (y // 2)) & 1,
    )
    opposite = x + 1 - 2 * (x % 2)
    reg_targets = (
        partner,
        device(opposite, y, k),
        device(opposite, y, 1 - k),
        device(SIDE - 1 - x, y, k),
        device(x, y + 1 - 2 * (y % 2), k),
        device(x, SIDE - 1 - y, k),
        partner,
    )

    def reg_copy(i):
        if i < 3:
            src, dst = regs_in.at[k if i == 1 else 1 - k], regs_pair[0].at[i + 1]
        elif i < REG_COPIES - 1:
            src, dst = regs_pair[i - 2].at[0], regs_pair[i - 2].at[1]
        else:
            src, dst = regs.at[k], regs.at[k]
        return remote(src, dst, reg_send.at[i], reg_recv.at[i], reg_targets[i])

    def reg_step(i):
        if i == 0:
            for c in range(2):
                load_regs(c).wait()
            for n in range(3):
                reg_copy(n).start()
            regs_pair[0][0] = regs_in[k]
            return
        for n in range(3) if i == 1 else (i + 1,):
            reg_copy(n).wait_recv()
        chosen = regs_pair[i - 1][sides[i - 1]]
        if i < REG_STEPS - 1:
            regs_pair[i][0] = chosen
        else:
            regs[k] = chosen
        reg_copy(i + 2).start()

    def regs_here():
        remote(
            regs.at[1 - k], regs.at[1 - k], reg_send.at[REG_COPIES - 1], reg_recv.at[REG_COPIES - 1], partner
        ).wait_recv()

    def give(u, f):
        ref = full_refs[u][f]
        offset = FULL[f][0]
        spot = device(
            (x - sign * offset[0] + SIDE) % SIDE, (y - sign * offset[1] + SIDE) % SIDE, k
        )
        for i, (_, before, way) in enumerate(LEAF):
            if before == f:
                turned = way + k if way % 2 == 0 else way - k
                for core in range(CORES):
                    outgoing[u, 2 * i + core] = ref[asks_s[2 * turned + core, 0, spot]]
        outgoing[u, 2 * LEAVES + f] = ref[asks_s[PARTNER, 0, spot]]
        if f:
            received[u][slot(k, offset)] = ref[asks_s[SELF, 0, spot]]
        for i, (_, before, _) in enumerate(LEAF):
            if before == f:
                for core in range(CORES):
                    leaf(u, i, core).start()
        across(u, f).start()

    def begin(u):
        load(u).wait()
        full(u, 1).start()
        full(u, 2).start()

    def stage(u, n):
        if not 0 <= u < UNITS:
            return
        if n == 0:
            give(u, 0)
        elif n == 1:
            for f in (1, 2):
                full(u, f).wait_recv()
                full(u, f + 2).start()
            give(u, 1)
            give(u, 2)
        elif n == 2:
            full(u, 3).wait_recv()
            full(u, 5).start()
            full(u, 4).wait_recv()
            give(u, 3)
            give(u, 4)
        else:
            full(u, 5).wait_recv()
            give(u, 5)

    def all_here(u):
        h, c = ORDER[u]
        ref = received[u].at[pl.ds(0, MESSAGES)]
        remote(ref, ref, unit_send.at[u], unit_recv.at[u], partner).wait_recv()
        if c == 0:
            load_q(h).wait()
            spare = regs[0, :, pl.ds(h * HEAD_SIZE, HEAD_SIZE)]
            received[u][slot(k, (0, 0))] = jnp.concatenate([spare, spare], axis=0)
        else:
            received[u][slot(k, (0, 0))] = jnp.zeros((rows, HEAD_SIZE), jnp.bfloat16)

    def store(h, b):
        return pltpu.make_async_copy(
            out_here.at[h * blocks + b],
            out_hbm.at[pl.ds(pl.multiple_of(b * rows, rows), rows), pl.ds(h * width, width)],
            out_sem.at[h * blocks + b],
        )

    def far_slots(b):
        places = []
        for t in range(slots):
            o = lists[b, t] >> 2
            used = flag(b, t)
            core = o & 1
            turn = 1 - 2 * core
            dx = ((x - (o >> 3)) * turn) & 3
            dy = ((y - (o >> 1)) * turn) & 3
            place = core * CHIP_SLOTS + dx * SIDE + dy
            places.append((place * used + slot(k, (0, 0)) * (1 - used), used))
        return places

    def keys_of(h, b, places):
        return key_pairs(
            full_refs[KEYS[h]][0][b],
            regs[0, :, pl.ds(h * HEAD_SIZE, HEAD_SIZE)],
            [received[KEYS[h]][place] for place, _ in places],
        )

    def values_of(h, b, places):
        return value_pairs(
            full_refs[VALUES[h]][0][b],
            regs[1, :, pl.ds(h * HEAD_SIZE, HEAD_SIZE)],
            [received[VALUES[h]][place] for place, _ in places],
            [marks[used] for _, used in places],
        )

    def queries_of(h, b):
        here = pl.ds(pl.multiple_of(b * rows, rows), rows)
        return stacked_heads(q_here[here, pl.ds(h * width, width)])

    part = rows * GROUP // PARTS

    def compute_weights(h):
        @pl.loop(0, blocks)
        def _(b):
            stacked = queries_of(h, b)
            keys = keys_of(h, b, far_slots(b))
            seen = seen_rows(rows, image[b])
            scores = [score(stacked, keys, seen, 0, part)]
            for n in range(PARTS):
                if n + 1 < PARTS:
                    scores.append(
                        score(stacked, keys, seen, (n + 1) * part, (n + 2) * part)
                    )
                for i, w in enumerate(soften(scores[n])):
                    weights_here[h % 2, b, i, pl.ds(n * part, part)] = w

    def compute_outputs(h):
        @pl.loop(0, blocks)
        def _(b):
            values = values_of(h, b, far_slots(b))
            pairs = len(values)
            outs = finish([weights_here[h % 2, b, i] for i in range(pairs)], values)
            out_here[h * blocks + b] = spread_heads(outs, rows)
            store(h, b).start()

    begin(0)
    reg_step(0)
    for u in range(1, LEAD):
        begin(u)
    others = asks.at[pl.ds(0, SELF)]
    remote(others, others, ask_send.at[0], ask_recv.at[0], partner).wait_recv()
    to_scalars = pltpu.make_async_copy(asks, asks_s, table_sem.at[0])
    to_scalars.start()
    to_scalars.wait()
    stage(0, 0)
    reg_step(1)
    for u in range(1, LEAD):
        stage(u, 0)
    for t in range(UNITS + 3):
        stage(t, 1)
        stage(t - 1, 2)
        stage(t - 2, 3)
        if t + LEAD < UNITS:
            begin(t + LEAD)
            stage(t + LEAD, 0)
        if t + 2 < REG_STEPS:
            reg_step(t + 2)
        elif t + 2 == REG_STEPS:
            regs_here()
        if t >= 3:
            h, c = ORDER[t - 3]
            all_here(t - 3)
            if c == 0:
                compute_weights(h)
            else:
                compute_outputs(h)

    remote(others, others, ask_send.at[0], ask_recv.at[0], partner).wait_send()
    for i in range(REG_COPIES):
        reg_copy(i).wait_send()
    for u in range(UNITS):
        sent = outgoing.at[u]
        remote(sent, sent, unit_send.at[u], unit_recv.at[u], partner).wait_send()
        sent = outgoing.at[u, pl.ds(0, (PLACES - 1) * blocks)]
        remote(sent, sent, full_send.at[u], unit_recv.at[u], partner).wait_send()
    for h in range(KEY_VALUE_HEADS):
        for b in range(blocks):
            store(h, b).wait()


def layer(q, k, v, lists, counts, image, owner):
    blocks, slots = lists.shape
    rows = q.shape[0] // blocks
    kv_width = k.shape[1]
    width = GROUP * HEAD_SIZE
    heads = KEY_VALUE_HEADS
    bf16 = jnp.bfloat16
    dma = pltpu.SemaphoreType.DMA
    return pl.pallas_call(
        layer_kernel,
        out_shape=jax.ShapeDtypeStruct(q.shape, bf16),
        in_specs=[pl.BlockSpec(memory_space=pl.ANY)] * 7,
        out_specs=pl.BlockSpec(memory_space=pl.ANY),
        scratch_shapes=[pltpu.SMEM(a.shape, jnp.int32) for a in (lists, counts, image, owner)]
        + [dma((4,))]
        + [pltpu.VMEM((blocks, rows, HEAD_SIZE), bf16)] * (UNITS * PLACES)
        + [pltpu.VMEM((CORES * CHIP_SLOTS, rows, HEAD_SIZE), bf16)] * UNITS
        + [pltpu.VMEM((4, REG, kv_width), bf16)]
        + [pltpu.VMEM((2, REG, kv_width), bf16)] * (REG_STEPS - 2)
        + [
            pltpu.VMEM((UNITS, 2 * LEAVES + PLACES, rows, HEAD_SIZE), bf16),
            pltpu.VMEM((ASKERS, 1, 128), jnp.int32),
            pltpu.SMEM((ASKERS, 1, 128), jnp.int32),
            pltpu.VMEM((2, rows, HEAD_SIZE), bf16),
            pltpu.VMEM((2, REG, kv_width), bf16),
            pltpu.VMEM((2, REG, kv_width), bf16),
            pltpu.VMEM(q.shape, bf16),
            pltpu.VMEM((heads * blocks, rows, width), bf16),
            pltpu.VMEM((2, blocks, (slots + 2) // 2, GROUP * rows, 2 * rows), bf16),
            dma((1,)),
            dma((UNITS,)),
            dma((2,)),
            dma((heads,)),
            dma((heads * blocks,)),
            dma((1,)),
            dma((1,)),
            dma((REG_COPIES,)),
            dma((REG_COPIES,)),
            dma((UNITS,)),
            dma((UNITS, PLACES)),
            dma((UNITS,)),
            dma((UNITS,)),
        ],
        compiler_params=pltpu.CompilerParams(
            collective_id=0, has_side_effects=True, vmem_limit_bytes=62 << 20
        ),
        name="layer",
    )(
        q,
        k.reshape(blocks, rows, kv_width),
        v.reshape(blocks, rows, kv_width),
        lists,
        counts,
        image,
        owner,
    )


def per_device(queries, keys, values, reg_owner, block_lists, list_counts, image_blocks):
    out = layer(
        queries[0],
        keys[0],
        values[0],
        block_lists[0],
        list_counts[0],
        image_blocks[0],
        reg_owner,
    )
    return out[None]


def solution(mesh):
    placed = (
        P("samp", "seq", None),
        P("samp", "seq", None),
        P("samp", "seq", None),
        P("samp"),
        P("samp", "seq", None),
        P("samp", "seq"),
        P("samp", "seq"),
    )
    return jax.shard_map(
        per_device, mesh=mesh, in_specs=placed, out_specs=P("samp", "seq", None), check_vma=False
    )
```
